32 devices in a mesh: dp: 1 (over z), tp: 32 (over x, y, core).
Axes of the slice: x: 4, y: 4, z: 1, core: 2. Of those that a mesh axis runs over, the one named last changes fastest.
The devices are a block of a 4x4x8 slice.
Arguments:
- x: bfloat16 [7168, 5120], P(('dp', 'tp'))
- w_gate: bfloat16 [5120, 32768], P(None, 'tp')
- w_up: bfloat16 [5120, 32768], P(None, 'tp')
- w_down: bfloat16 [32768, 5120], P('tp')
Outputs:
- output: bfloat16 [7168, 5120], P(('dp', 'tp'))
All inputs are finite; a program needn't handle non-finite values.
Results may differ from the reference program's by a relative error of at most 0.016.
Values are sent between devices in bfloat16 or wider.
A program may use at most 768 MiB of HBM per device.

```python
import jax
import jax.numpy as jnp

ROWS = 7168
D = 5120
FF = 32768


def setup_inputs(seed: int = 0, part: int = 0) -> dict:
    kx, kg, ku, kd = jax.random.split(jax.random.key(seed), 4)
    drawn = {
        "x": jax.random.normal(jax.random.fold_in(kx, part), (ROWS, D), jnp.float32),
        "w_gate": jax.random.normal(kg, (D, FF), jnp.float32) * D**-0.5,
        "w_up": jax.random.normal(ku, (D, FF), jnp.float32) * D**-0.5,
        "w_down": jax.random.normal(kd, (FF, D), jnp.float32) * FF**-0.5,
    }
    return {k: v.astype(jnp.bfloat16) for k, v in drawn.items()}


def reference(x, w_gate, w_up, w_down):
    gate = jnp.dot(x, w_gate, preferred_element_type=jnp.float32)
    up = jnp.dot(x, w_up, preferred_element_type=jnp.float32)
    hidden = (jax.nn.silu(gate) * up).astype(jnp.bfloat16)
    return jnp.dot(hidden, w_down, preferred_element_type=jnp.float32).astype(jnp.bfloat16)
```

```python
import functools
import math

import jax
import jax.numpy as jnp
from jax import lax
from jax.experimental import pallas as pl
from jax.experimental.pallas import tpu as pltpu
from jax.sharding import PartitionSpec as P

MESH = pl.DeviceIdType.MESH
BF16 = jnp.bfloat16
F32 = jnp.float32


def neighbours(tp, side):
    core, chip = tp % 2, tp // 2
    x, y = chip // side, chip % side
    last = ((x + y) % side + 1) // side
    first = (side - (x + y) % side) // side

    def at(u, v):
        return (u * side + v) * 2 + core

    a = (at((x + last) % side, (y + 1 - last) % side), at((x + side - first) % side, (y + side - 1 + first) % side))
    b = (at((x + 1 - last) % side, (y + last) % side), at((x + side - 1 + first) % side, (y + side - first) % side))
    turn = lambda p: (p[0] + core * (p[1] - p[0]), p[1] + core * (p[0] - p[1]))
    return turn(a), turn(b), tp + 1 - 2 * core


def kernel(
    cfg,
    x_ref, wg_ref, wu_ref, wd_ref,
    y_ref, xg_ref, xp_ref,
    wg, wu, wd, xv, hid, run, pt, out, outp,
    w_sem, xv_sem, y_sem, ag_send, ag_recv, xp_send, xp_recv, run_send, run_recv, pt_send, pt_recv, run_free, pt_free,
):
    side, n, na, nb = cfg
    rows = x_ref.shape[0]
    half = rows // 2
    pieces = out.shape[1]
    dp, tp = lax.axis_index("dp"), lax.axis_index("tp")
    ring_a, ring_b, partner = neighbours(tp, side)
    rings = (ring_a, ring_b)

    def to(t):
        return dict(device_id=(dp, t), device_id_type=MESH)

    barrier = pltpu.get_barrier_semaphore()
    for t in (*ring_a, *ring_b, partner):
        pl.semaphore_signal(barrier, inc=1, **to(t))

    loads = [pltpu.make_async_copy(s, d, w_sem.at[i]) for i, (s, d) in enumerate(((wg_ref, wg), (wu_ref, wu), (wd_ref, wd)))]
    for c in loads:
        c.start()
    run[0] = jnp.zeros_like(run[0])
    pl.semaphore_wait(barrier, 5)

    def span(r):
        return pl.ds(r * half, half)

    def gather(d, r, src=None):
        return pltpu.make_async_remote_copy(
            (xg_ref.at[d, span(r)] if src is None else src.at[span(r)]), xg_ref.at[d + 1, span(r)],
            ag_send.at[d, r], ag_recv.at[d + 1, r], **to(rings[r][0]),
        )

    def share(d, src=None):
        return pltpu.make_async_remote_copy(
            xg_ref.at[d] if src is None else src, xp_ref.at[d], xp_send.at[d], xp_recv.at[d], **to(partner)
        )

    def load_own(d):
        return pltpu.make_async_copy(xg_ref.at[d], xv.at[1], xv_sem.at[1])

    def load_partner(d):
        return pltpu.make_async_copy(xp_ref.at[d], xv.at[0], xv_sem.at[0])

    def pass_sum(s, p, r):
        return pltpu.make_async_remote_copy(
            out.at[s, p, span(r)], run.at[1 - s, p, span(r)], run_send.at[s, p, r], run_recv.at[1 - s, p, r], **to(rings[r][0])
        )

    def got_sum(s, p, r):
        return pltpu.make_async_remote_copy(
            out.at[s, p, span(r)], run.at[s, p, span(r)], run_send.at[s, p, r], run_recv.at[s, p, r], **to(rings[r][0])
        )

    def pass_term(s, p):
        return pltpu.make_async_remote_copy(outp.at[s, p], pt.at[s, p], pt_send.at[s, p], pt_recv.at[s, p], **to(partner))

    def write_y(p):
        return pltpu.make_async_copy(out.at[1, p], y_ref.at[:, pl.ds(pl.multiple_of(p * nb, nb), nb)], y_sem.at[p])

    def up(slot):
        @pl.loop(0, hid.shape[1] // na)
        def _(i):
            c = pl.ds(pl.multiple_of(i * na, na), na)
            gate = jnp.dot(xv[slot], wg[:, c], preferred_element_type=F32)
            up = jnp.dot(xv[slot], wu[:, c], preferred_element_type=F32)
            hid[:, c] = (jax.nn.silu(gate) * up).astype(BF16)

    def down(p):
        c = pl.ds(pl.multiple_of(p * nb, nb), nb)
        return jnp.dot(hid[...], wd[:, c], preferred_element_type=F32)

    for r in range(2):
        gather(0, r, x_ref).start()
    share(n, x_ref).start()
    for r in range(2):
        gather(0, r).wait_recv()
        gather(1, r).start()
    share(1).start()
    load_own(1).start()
    share(1).wait_recv()
    load_partner(1).start()
    for c in loads:
        c.wait()

    @pl.loop(0, n)
    def _(q):
        d = q + 1
        s = q % 2
        load_partner(0).wait()
        up(0)

        @pl.when(d + 1 < n)
        def _():
            for r in range(2):
                gather(d, r).wait_recv()

            @pl.when(d + 2 < n)
            def _():
                for r in range(2):
                    gather(d + 1, r).start()

            share(d + 1).start()

        @pl.when(q >= 2)
        def _():
            pl.semaphore_wait(pt_free, 1)

        @pl.loop(0, pieces)
        def _(p):
            @pl.when(q >= 2)
            def _():
                pass_term(s, p).wait_send()

            outp[s, p] = down(p).astype(BF16)
            pass_term(s, p).start()

        load_own(0).wait()
        up(1)

        @pl.when(d + 1 < n)
        def _():
            load_own(d + 1).start()

        @pl.when(d + 1 == n)
        def _():
            pltpu.make_async_copy(x_ref, xv.at[1], xv_sem.at[1]).start()

        @pl.when(d < n)
        def _():
            share(d + 1, x_ref).wait_recv()
            load_partner(d + 1).start()

        @pl.when((q >= 1) & (d < n))
        def _():
            for r in range(2):
                pl.semaphore_wait(run_free.at[r], 1)

        @pl.loop(0, pieces)
        def _(p):
            @pl.when(q >= 2)
            def _():
                for r in range(2):
                    pass_sum(s, p, r).wait_send()

            @pl.when(q >= 1)
            def _():
                for r in range(2):
                    got_sum(s, p, r).wait_recv()

            pass_term(s, p).wait_recv()
            out[s, p] = (down(p) + run[s, p].astype(F32) + pt[s, p].astype(F32)).astype(BF16)

            @pl.when(d < n)
            def _():
                for r in range(2):
                    pass_sum(s, p, r).start()

            @pl.when(d == n)
            def _():
                write_y(p).start()

        @pl.when(q < n - 2)
        def _():
            for r in range(2):
                pl.semaphore_signal(run_free.at[r], inc=1, **to(rings[r][1]))
            pl.semaphore_signal(pt_free, inc=1, **to(partner))

    @pl.loop(0, pieces)
    def _(p):
        write_y(p).wait()
        for s in range(2):
            pass_term(s, p).wait_send()
        for r in range(2):
            pass_sum(0, p, r).wait_send()

    @pl.loop(0, n - 1)
    def _(d):
        for r in range(2):
            gather(d, r).wait_send()
        share(d + 1).wait_send()

    share(n, x_ref).wait_send()


def solution(mesh):
    group = mesh.shape["tp"]
    n = group // 2
    side = math.isqrt(n)

    def step(x, w_gate, w_up, w_down):
        rows, depth = x.shape
        width = w_gate.shape[1]
        na, nb = width // 2, depth // 5
        pieces = depth // nb
        hbm = pl.BlockSpec(memory_space=pltpu.HBM)
        part = pltpu.VMEM((2, pieces, rows, nb), BF16)
        dma = pltpu.SemaphoreType.DMA
        flops = 6 * group * rows * depth * width
        y, _, _ = pl.pallas_call(
            functools.partial(kernel, (side, n, na, nb)),
            out_shape=(
                jax.ShapeDtypeStruct((rows, depth), BF16),
                jax.ShapeDtypeStruct((n, rows, depth), BF16),
                jax.ShapeDtypeStruct((n + 1, rows, depth), BF16),
            ),
            in_specs=[hbm] * 4,
            out_specs=(hbm,) * 3,
            scratch_shapes=[
                pltpu.VMEM((depth, width), BF16),
                pltpu.VMEM((depth, width), BF16),
                pltpu.VMEM((width, depth), BF16),
                pltpu.VMEM((2, rows, depth), BF16),
                pltpu.VMEM((rows, width), BF16),
                part, part, part, part,
                dma((3,)), dma((2,)), dma((pieces,)),
                dma((n, 2)), dma((n, 2)), dma((n + 1,)), dma((n + 1,)),
                dma((2, pieces, 2)), dma((2, pieces, 2)), dma((2, pieces)), dma((2, pieces)),
                pltpu.SemaphoreType.REGULAR((2,)), pltpu.SemaphoreType.REGULAR,
            ],
            compiler_params=pltpu.CompilerParams(
                collective_id=0, has_side_effects=True, vmem_limit_bytes=63 * 2**20
            ),
            cost_estimate=pl.CostEstimate(flops=flops, bytes_accessed=4 * group * rows * depth, transcendentals=0),
            name="mlp",
        )(x, w_gate, w_up, w_down)
        return y

    return jax.shard_map(
        step,
        mesh=mesh,
        in_specs=(P(("dp", "tp"), None), P(None, "tp"), P(None, "tp"), P("tp", None)),
        out_specs=P(("dp", "tp"), None),
        check_vma=False,
    )
```

```python
import functools
import math

import jax
import jax.numpy as jnp
from jax import lax
from jax.experimental import pallas as pl
from jax.experimental.pallas import tpu as pltpu
from jax.sharding import PartitionSpec as P

MESH = pl.DeviceIdType.MESH
BF16 = jnp.bfloat16
F32 = jnp.float32
PARTS = 2
PIECES = 5
SPARE = 4


def neighbours(tp, side):
    core, chip = tp % 2, tp // 2
    x, y = chip // side, chip % side
    last = ((x + y) % side + 1) // side
    first = (side - (x + y) % side) // side

    def at(u, v):
        return (u * side + v) * 2 + core

    a = (at((x + last) % side, (y + 1 - last) % side), at((x + side - first) % side, (y + side - 1 + first) % side))
    b = (at((x + 1 - last) % side, (y + last) % side), at((x + side - 1 + first) % side, (y + side - first) % side))
    turn = lambda p: (p[0] + core * (p[1] - p[0]), p[1] + core * (p[0] - p[1]))
    return turn(a), turn(b), tp + 1 - 2 * core


def kernel(
    n, side,
    x_ref, wg_ref, wu_ref, wd_ref,
    y_ref, xg_ref, xp_ref,
    wg, wu, wd, xo, xp, hid, run, pt, out, outp,
    w_sem, xo_sem, xp_sem, y_sem, ag_send, ag_recv, sh_send, sh_recv, run_send, run_recv, pt_send, pt_recv, run_free, pt_free,
):
    rows, depth = x_ref.shape
    half = rows // 2
    na, nb, nc = hid.shape[2] // PARTS, depth // PIECES, depth // PARTS
    dp, tp = lax.axis_index("dp"), lax.axis_index("tp")
    ring_a, ring_b, partner = neighbours(tp, side)
    rings = (ring_a, ring_b)

    def to(t):
        return dict(device_id=(dp, t), device_id_type=MESH)

    def span(r):
        return pl.ds(r * half, half)

    def cols(i, size):
        return pl.ds(pl.multiple_of(i * size, size), size)

    def gather(d, g, r, src=None):
        return pltpu.make_async_remote_copy(
            (xg_ref.at[d] if src is None else src).at[span(r), cols(g, nc)], xg_ref.at[d + 1, span(r), cols(g, nc)],
            ag_send.at[d, g, r], ag_recv.at[d + 1, g, r], **to(rings[r][0]),
        )

    def share(d, g, src=None):
        return pltpu.make_async_remote_copy(
            (xg_ref.at[d] if src is None else src).at[:, cols(g, nc)], xp_ref.at[d, :, cols(g, nc)],
            sh_send.at[d, g], sh_recv.at[d, g], **to(partner),
        )

    def load_own(d, src=None):
        return pltpu.make_async_copy(xg_ref.at[d] if src is None else src, xo.at[d % 2], xo_sem.at[d % 2])

    def load_partner(d):
        return pltpu.make_async_copy(xp_ref.at[d], xp, xp_sem)

    def pass_sum(q, p, r):
        s, t = q % 2, (q + 1) % 2
        return pltpu.make_async_remote_copy(
            out.at[s, p, span(r)], run.at[t, p, span(r)], run_send.at[s, p, r], run_recv.at[t, p, r], **to(rings[r][0])
        )

    def pass_term(s, t, p):
        return pltpu.make_async_remote_copy(outp.at[s, p], pt.at[t, p], pt_send.at[s, p], pt_recv.at[t, p], **to(partner))

    def write_y(p):
        return pltpu.make_async_copy(out.at[0, p], y_ref.at[:, cols(p, nb)], y_sem.at[p])

    def up(x, slot, between=None):
        @pl.loop(0, PARTS)
        def _(i):
            c = cols(i, na)
            gate = jnp.dot(x[...], wg[:, c], preferred_element_type=F32)
            up = jnp.dot(x[...], wu[:, c], preferred_element_type=F32)
            hid[slot, :, c] = (jax.nn.silu(gate) * up).astype(BF16)
            if between is not None:
                between(i)

    def down(slot, p):
        return jnp.dot(hid[slot], wd[:, cols(p, nb)], preferred_element_type=F32)

    barrier = pltpu.get_barrier_semaphore()
    for t in (*ring_a, *ring_b, partner):
        pl.semaphore_signal(barrier, inc=1, **to(t))
    loads = [pltpu.make_async_copy(s, d, w_sem.at[i]) for i, (s, d) in enumerate(((wg_ref, wg), (wu_ref, wu), (wd_ref, wd)))]
    for c in loads:
        c.start()
    pl.semaphore_wait(barrier, 5)

    for g in range(PARTS):
        for r in range(2):
            gather(0, g, r, x_ref).start()
    for g in range(PARTS):
        share(0, g, x_ref).start()
    run[1] = jnp.zeros_like(run[1])
    for g in range(PARTS):
        share(0, g, x_ref).wait_recv()
    load_partner(0).start()
    loads[0].wait()
    loads[1].wait()

    @pl.loop(0, n + 1)
    def _(q):
        s = q % 2

        @pl.when(q < n)
        def _():
            load_partner(0).wait()

            def between(g):
                @pl.when(q + 1 < n)
                def _():
                    for r in range(2):
                        gather(q, g, r).wait_recv()

                    @pl.when(q + 2 < n)
                    def _():
                        for r in range(2):
                            gather(q + 1, g, r).start()

                    share(q + 1, g).start()

            up(xp, 3, between)

            @pl.when(q + 1 < n)
            def _():
                load_own(q + 1).start()

            @pl.when(q == 0)
            def _():
                loads[2].wait()

            @pl.when(q >= 3)
            def _():
                pl.semaphore_wait(pt_free, 1)

            t = jnp.where(q == 0, 2, s)

            @pl.loop(0, PIECES)
            def _(p):
                @pl.when(q >= 2)
                def _():
                    pass_term(s, 0, p).wait_send()

                outp[s, p] = down(3, p).astype(BF16)
                pass_term(s, t, p).start()

        @pl.when(q == SPARE)
        def _():
            load_own(0, x_ref).start()

        @pl.when((q >= 1) & (q < n - 1))
        def _():
            @pl.loop(q + jnp.minimum(q // 3, 1), q + 1 + jnp.minimum(q // 2, 1))
            def _(u):
                load_own(u, x_ref).wait()
                up(xo.at[u % 2], u % 2)

        @pl.when(q == SPARE)
        def _():
            load_own(0, x_ref).wait()
            up(xo.at[0], 2)

        @pl.when(q + 1 < n)
        def _():
            for g in range(PARTS):
                share(q + 1, g).wait_recv()
            load_partner(q + 1).start()

        @pl.when(q >= 1)
        def _():
            t = jnp.where(q == n, 2, s)

            @pl.when((q >= 2) & (q < n))
            def _():
                for r in range(2):
                    pl.semaphore_wait(run_free.at[r], 1)

            @pl.loop(0, PIECES)
            def _(p):
                @pl.when(q >= 3)
                def _():
                    for r in range(2):
                        pass_sum(q, p, r).wait_send()

                @pl.when(q >= 2)
                def _():
                    for r in range(2):
                        pass_sum(q + 1, p, r).wait_recv()

                pass_term(s, t, p).wait_recv()
                out[s, p] = (down(t, p) + run[s, p].astype(F32) + pt[t, p].astype(F32)).astype(BF16)

                @pl.when(q < n)
                def _():
                    for r in range(2):
                        pass_sum(q, p, r).start()

                @pl.when(q == n)
                def _():
                    write_y(p).start()

            @pl.when(q < n - 1)
            def _():
                for r in range(2):
                    pl.semaphore_signal(run_free.at[r], inc=1, **to(rings[r][1]))

            @pl.when(q < n - 2)
            def _():
                pl.semaphore_signal(pt_free, inc=1, **to(partner))

    @pl.loop(0, PIECES)
    def _(p):
        write_y(p).wait()
        for s in range(2):
            pass_term(s, 0, p).wait_send()
        for r in range(2):
            pass_sum(n - 1, p, r).wait_send()

    @pl.loop(0, n)
    def _(d):
        for g in range(PARTS):
            share(d, g).wait_send()

            @pl.when(d < n - 1)
            def _():
                for r in range(2):
                    gather(d, g, r).wait_send()


def solution(mesh):
    n = mesh.shape["tp"] // 2
    side = math.isqrt(n)

    def step(x, w_gate, w_up, w_down):
        rows, depth = x.shape
        width = w_gate.shape[1]
        hbm = pl.BlockSpec(memory_space=pltpu.HBM)
        dma, flag = pltpu.SemaphoreType.DMA, pltpu.SemaphoreType.REGULAR

        def sums(slots):
            return pltpu.VMEM((slots, PIECES, rows, depth // PIECES), BF16)

        y, _, _ = pl.pallas_call(
            functools.partial(kernel, n, side),
            out_shape=(
                jax.ShapeDtypeStruct((rows, depth), BF16),
                jax.ShapeDtypeStruct((n, rows, depth), BF16),
                jax.ShapeDtypeStruct((n, rows, depth), BF16),
            ),
            in_specs=[hbm] * 4,
            out_specs=(hbm,) * 3,
            scratch_shapes=[
                pltpu.VMEM((depth, width), BF16),
                pltpu.VMEM((depth, width), BF16),
                pltpu.VMEM((width, depth), BF16),
                pltpu.VMEM((2, rows, depth), BF16),
                pltpu.VMEM((rows, depth), BF16),
                pltpu.VMEM((4, rows, width), BF16),
                sums(2), sums(3), sums(2), sums(2),
                dma((3,)), dma((2,)), dma, dma((PIECES,)),
                dma((n, PARTS, 2)), dma((n, PARTS, 2)), dma((n, PARTS)), dma((n, PARTS)),
                dma((2, PIECES, 2)), dma((2, PIECES, 2)), dma((2, PIECES)), dma((3, PIECES)),
                flag((2,)), flag,
            ],
            compiler_params=pltpu.CompilerParams(collective_id=0, has_side_effects=True, vmem_limit_bytes=63 * 2**20),
            cost_estimate=pl.CostEstimate(
                flops=6 * 2 * n * rows * depth * width, bytes_accessed=8 * 2 * n * rows * depth, transcendentals=0
            ),
            name="mlp",
        )(x, w_gate, w_up, w_down)
        return y

    return jax.shard_map(
        step,
        mesh=mesh,
        in_specs=(P(("dp", "tp"), None), P(None, "tp"), P(None, "tp"), P("tp", None)),
        out_specs=P(("dp", "tp"), None),
        check_vma=False,
    )
```

```python
import functools
import math

import jax
import jax.numpy as jnp
from jax import lax
from jax.experimental import pallas as pl
from jax.experimental.pallas import tpu as pltpu
from jax.sharding import PartitionSpec as P

MESH = pl.DeviceIdType.MESH
BF16 = jnp.bfloat16
F32 = jnp.float32
PARTS = 2
PIECES = 5
SPARE = 4


def neighbours(tp, side):
    core, chip = tp % 2, tp // 2
    x, y = chip // side, chip % side
    last = ((x + y) % side + 1) // side
    first = (side - (x + y) % side) // side

    def at(u, v):
        return (u * side + v) * 2 + core

    a = (at((x + last) % side, (y + 1 - last) % side), at((x + side - first) % side, (y + side - 1 + first) % side))
    b = (at((x + 1 - last) % side, (y + last) % side), at((x + side - 1 + first) % side, (y + side - first) % side))
    turn = lambda p: (p[0] + core * (p[1] - p[0]), p[1] + core * (p[0] - p[1]))
    return turn(a), turn(b), tp + 1 - 2 * core


def kernel(
    n, side,
    x_ref, wg_ref, wu_ref, wd_ref,
    y_ref, xg_ref, xp_ref, pt0_ref,
    wg, wu, wd, xo, xp, hid, run, pt, out, outp,
    w_sem, xo_sem, xp_sem, pt0_sem, ag_send, ag_recv, sh_send, sh_recv, run_send, run_recv, pt_send, pt_recv, run_free, pt_free,
):
    rows, depth = x_ref.shape
    half = rows // 2
    na, nb, nc = hid.shape[2] // PARTS, depth // PIECES, depth // PARTS
    dp, tp = lax.axis_index("dp"), lax.axis_index("tp")
    ring_a, ring_b, partner = neighbours(tp, side)
    rings = (ring_a, ring_b)

    def to(t):
        return dict(device_id=(dp, t), device_id_type=MESH)

    def span(r):
        return pl.ds(r * half, half)

    def cols(i, size):
        return pl.ds(pl.multiple_of(i * size, size), size)

    def gather(d, g, r, src=None):
        return pltpu.make_async_remote_copy(
            (xg_ref.at[d] if src is None else src).at[span(r), cols(g, nc)], xg_ref.at[d + 1, span(r), cols(g, nc)],
            ag_send.at[d, g, r], ag_recv.at[d + 1, g, r], **to(rings[r][0]),
        )

    def share(d, g, src=None):
        return pltpu.make_async_remote_copy(
            (xg_ref.at[d] if src is None else src).at[:, cols(g, nc)], xp_ref.at[d, :, cols(g, nc)],
            sh_send.at[d, g], sh_recv.at[d, g], **to(partner),
        )

    def load_own(d, src=None):
        return pltpu.make_async_copy(xg_ref.at[d] if src is None else src, xo, xo_sem)

    def load_partner(d):
        return pltpu.make_async_copy(xp_ref.at[d], xp, xp_sem)

    def pass_sum(q, p, r):
        t = (q + 1) % 2
        return pltpu.make_async_remote_copy(
            out.at[p, span(r)], run.at[t, p, span(r)], run_send.at[p, r], run_recv.at[t, p, r], **to(rings[r][0])
        )

    def pass_term(t, p):
        return pltpu.make_async_remote_copy(outp.at[p], pt.at[t, p], pt_send.at[p], pt_recv.at[t, p], **to(partner))

    def pass_first(p):
        return pltpu.make_async_remote_copy(outp.at[p], pt0_ref.at[p], pt_send.at[p], pt_recv.at[2, p], **to(partner))

    def load_first():
        return pltpu.make_async_copy(pt0_ref, pt.at[0], pt0_sem)

    def up(x, slot, between=None):
        @pl.loop(0, PARTS)
        def _(i):
            c = cols(i, na)
            gate = jnp.dot(x[...], wg[:, c], preferred_element_type=F32)
            up = jnp.dot(x[...], wu[:, c], preferred_element_type=F32)
            hid[slot, :, c] = (jax.nn.silu(gate) * up).astype(BF16)
            if between is not None:
                between(i)

    def down(slot, p):
        return jnp.dot(hid[slot], wd[:, cols(p, nb)], preferred_element_type=F32)

    barrier = pltpu.get_barrier_semaphore()
    for t in (*ring_a, *ring_b, partner):
        pl.semaphore_signal(barrier, inc=1, **to(t))
    loads = [pltpu.make_async_copy(s, d, w_sem.at[i]) for i, (s, d) in enumerate(((wg_ref, wg), (wu_ref, wu), (wd_ref, wd)))]
    for c in loads:
        c.start()
    pl.semaphore_wait(barrier, 5)

    for g in range(PARTS):
        for r in range(2):
            gather(0, g, r, x_ref).start()
    for g in range(PARTS):
        share(0, g, x_ref).start()
    run[1] = jnp.zeros_like(run[1])
    for g in range(PARTS):
        share(0, g, x_ref).wait_recv()
    load_partner(0).start()
    loads[0].wait()
    loads[1].wait()

    @pl.loop(0, n + 1)
    def _(q):
        s = q % 2

        @pl.when(q < n)
        def _():
            load_partner(0).wait()

            def between(g):
                @pl.when(q + 1 < n)
                def _():
                    for r in range(2):
                        gather(q, g, r).wait_recv()

                    @pl.when(q + 2 < n)
                    def _():
                        for r in range(2):
                            gather(q + 1, g, r).start()

                    share(q + 1, g).start()

            up(xp, 3, between)

            @pl.when((q == 0) | (q >= 3) & (q + 1 < n))
            def _():
                load_own(q + 1).start()

            @pl.when(q == 0)
            def _():
                loads[2].wait()

            @pl.when(q >= 3)
            def _():
                pl.semaphore_wait(pt_free, 1)

            @pl.loop(0, PIECES)
            def _(p):
                @pl.when(q >= 1)
                def _():
                    pass_term(0, p).wait_send()

                outp[p] = down(3, p).astype(BF16)

                @pl.when(q == 0)
                def _():
                    pass_first(p).start()

                @pl.when(q >= 1)
                def _():
                    pass_term(s, p).start()

        @pl.when((q >= 1) & (q < n - 1))
        def _():
            @pl.loop(q + jnp.minimum(q // 3, 1), q + 1 + jnp.minimum(q // 2, 1))
            def _(u):
                load_own(0, x_ref).wait()
                up(xo, u % 2)

                @pl.when(u <= 2)
                def _():
                    load_own(u + 1).start()

        @pl.when(q == SPARE)
        def _():
            load_own(0, x_ref).start()
            load_own(0, x_ref).wait()
            up(xo, 2)

        @pl.when(q + 1 < n)
        def _():
            for g in range(PARTS):
                share(q + 1, g).wait_recv()
            load_partner(q + 1).start()

        @pl.when(q >= 1)
        def _():
            h = jnp.where(q == n, 2, s)

            @pl.when(q == n)
            def _():
                load_first().wait()

            @pl.when((q >= 2) & (q < n))
            def _():
                for r in range(2):
                    pl.semaphore_wait(run_free.at[r], 1)

            @pl.loop(0, PIECES)
            def _(p):
                @pl.when((q >= 2) & (q < n))
                def _():
                    for r in range(2):
                        pass_sum(q, p, r).wait_send()

                @pl.when(q >= 2)
                def _():
                    for r in range(2):
                        pass_sum(q + 1, p, r).wait_recv()

                @pl.when(q < n)
                def _():
                    pass_term(s, p).wait_recv()

                total = (down(h, p) + run[s, p].astype(F32) + pt[s, p].astype(F32)).astype(BF16)

                @pl.when(q < n)
                def _():
                    out[p] = total
                    for r in range(2):
                        pass_sum(q, p, r).start()

                @pl.when(q == n)
                def _():
                    y_ref[:, cols(p, nb)] = total

            @pl.when(q < n - 1)
            def _():
                for r in range(2):
                    pl.semaphore_signal(run_free.at[r], inc=1, **to(rings[r][1]))

            @pl.when(q < n - 2)
            def _():
                pl.semaphore_signal(pt_free, inc=1, **to(partner))

            @pl.when(q == n - 2)
            def _():
                for p in range(PIECES):
                    pass_first(p).wait_recv()
                load_first().start()

    @pl.loop(0, PIECES)
    def _(p):
        pass_term(0, p).wait_send()
        for r in range(2):
            pass_sum(n - 1, p, r).wait_send()

    @pl.loop(0, n)
    def _(d):
        for g in range(PARTS):
            share(d, g).wait_send()

            @pl.when(d < n - 1)
            def _():
                for r in range(2):
                    gather(d, g, r).wait_send()


def solution(mesh):
    n = mesh.shape["tp"] // 2
    side = math.isqrt(n)

    def step(x, w_gate, w_up, w_down):
        rows, depth = x.shape
        width = w_gate.shape[1]
        hbm = pl.BlockSpec(memory_space=pltpu.HBM)
        dma, flag = pltpu.SemaphoreType.DMA, pltpu.SemaphoreType.REGULAR

        def sums(*slots):
            return pltpu.VMEM((*slots, PIECES, rows, depth // PIECES), BF16)

        y, *_ = pl.pallas_call(
            functools.partial(kernel, n, side),
            out_shape=(
                jax.ShapeDtypeStruct((rows, depth), BF16),
                jax.ShapeDtypeStruct((n, rows, depth), BF16),
                jax.ShapeDtypeStruct((n, rows, depth), BF16),
                jax.ShapeDtypeStruct((PIECES, rows, depth // PIECES), BF16),
            ),
            in_specs=[hbm] * 4,
            out_specs=(pl.BlockSpec(memory_space=pltpu.VMEM), hbm, hbm, hbm),
            scratch_shapes=[
                pltpu.VMEM((depth, width), BF16),
                pltpu.VMEM((depth, width), BF16),
                pltpu.VMEM((width, depth), BF16),
                pltpu.VMEM((rows, depth), BF16),
                pltpu.VMEM((rows, depth), BF16),
                pltpu.VMEM((4, rows, width), BF16),
                sums(2), sums(2), sums(), sums(),
                dma((3,)), dma, dma, dma,
                dma((n, PARTS, 2)), dma((n, PARTS, 2)), dma((n, PARTS)), dma((n, PARTS)),
                dma((PIECES, 2)), dma((2, PIECES, 2)), dma((PIECES,)), dma((3, PIECES)),
                flag((2,)), flag,
            ],
            compiler_params=pltpu.CompilerParams(collective_id=0, has_side_effects=True, vmem_limit_bytes=int(51.6 * 2**20)),
            cost_estimate=pl.CostEstimate(
                flops=6 * 2 * n * rows * depth * width, bytes_accessed=8 * 2 * n * rows * depth, transcendentals=0
            ),
            name="mlp",
        )(x, w_gate, w_up, w_down)
        return y

    return jax.shard_map(
        step,
        mesh=mesh,
        in_specs=(P(("dp", "tp"), None), P(None, "tp"), P(None, "tp"), P("tp", None)),
        out_specs=P(("dp", "tp"), None),
        check_vma=False,
    )
```

```python
import functools
import math

import jax
import jax.numpy as jnp
from jax import lax
from jax.experimental import pallas as pl
from jax.experimental.pallas import tpu as pltpu
from jax.sharding import PartitionSpec as P

MESH = pl.DeviceIdType.MESH
BF16 = jnp.bfloat16
F32 = jnp.float32
PARTS = 2
PIECES = 5
SPARE = 4


def neighbours(tp, side):
    core, chip = tp % 2, tp // 2
    x, y = chip // side, chip % side
    last = ((x + y) % side + 1) // side
    first = (side - (x + y) % side) // side

    def at(u, v):
        return (u * side + v) * 2 + core

    a = (at((x + last) % side, (y + 1 - last) % side), at((x + side - first) % side, (y + side - 1 + first) % side))
    b = (at((x + 1 - last) % side, (y + last) % side), at((x + side - 1 + first) % side, (y + side - first) % side))
    turn = lambda p: (p[0] + core * (p[1] - p[0]), p[1] + core * (p[0] - p[1]))
    return turn(a), turn(b), tp + 1 - 2 * core


def kernel(
    n, side,
    x_ref, wg_ref, wu_ref, wd_ref,
    y_ref, xg_ref, xp_ref, pt0_ref,
    wg, wu, wd, xo, xp, hid, run, pt, out, outp,
    w_sem, xo_sem, xp_sem, pt0_sem, ag_send, ag_recv, sh_send, sh_recv, run_send, run_recv, pt_send, pt_recv, run_free, pt_free,
):
    rows, depth = x_ref.shape
    half = rows // 2
    na, nb, nc = hid.shape[2] // PARTS, depth // PIECES, depth // PARTS
    dp, tp = lax.axis_index("dp"), lax.axis_index("tp")
    ring_a, ring_b, partner = neighbours(tp, side)
    rings = (ring_a, ring_b)

    def to(t):
        return dict(device_id=(dp, t), device_id_type=MESH)

    def span(r):
        return pl.ds(r * half, half)

    def cols(i, size):
        return pl.ds(pl.multiple_of(i * size, size), size)

    def gather(d, g, r, src=None):
        return pltpu.make_async_remote_copy(
            (xg_ref.at[d] if src is None else src).at[span(r), cols(g, nc)], xg_ref.at[d + 1, span(r), cols(g, nc)],
            ag_send.at[d, g, r], ag_recv.at[d + 1, g, r], **to(rings[r][0]),
        )

    def share(d, g, src=None):
        return pltpu.make_async_remote_copy(
            (xg_ref.at[d] if src is None else src).at[:, cols(g, nc)], xp_ref.at[d, :, cols(g, nc)],
            sh_send.at[d, g], sh_recv.at[d, g], **to(partner),
        )

    def load_own(d, src=None):
        return pltpu.make_async_copy(xg_ref.at[d] if src is None else src, xo, xo_sem)

    def load_partner(d):
        return pltpu.make_async_copy(xp_ref.at[d], xp, xp_sem)

    def pass_sum(q, p, r):
        t = (q + 1) % 2
        return pltpu.make_async_remote_copy(
            out.at[p, span(r)], run.at[t, p, span(r)], run_send.at[p, r], run_recv.at[t, p, r], **to(rings[r][0])
        )

    def pass_term(t, p):
        return pltpu.make_async_remote_copy(outp.at[p], pt.at[t, p], pt_send.at[p], pt_recv.at[t, p], **to(partner))

    def pass_first(p):
        return pltpu.make_async_remote_copy(outp.at[p], pt0_ref.at[p], pt_send.at[p], pt_recv.at[2, p], **to(partner))

    def load_first():
        return pltpu.make_async_copy(pt0_ref, pt.at[0], pt0_sem)

    def up(x, slot, i):
        c = cols(i, na)
        gate = jnp.dot(x[...], wg[:, c], preferred_element_type=F32)
        up = jnp.dot(x[...], wu[:, c], preferred_element_type=F32)
        hid[slot, :, c] = (jax.nn.silu(gate) * up).astype(BF16)

    def advance(d, g):
        @pl.when(d < n)
        def _():
            for r in range(2):
                gather(d - 1, g, r).wait_recv()

            @pl.when(d + 1 < n)
            def _():
                for r in range(2):
                    gather(d, g, r).start()

            share(d, g).start()

    def await_partner(d):
        for g in range(PARTS):
            share(d, g).wait_recv()
        load_partner(d).start()

    def down(slot, p):
        return jnp.dot(hid[slot], wd[:, cols(p, nb)], preferred_element_type=F32)

    barrier = pltpu.get_barrier_semaphore()
    for t in (ring_a[1], ring_b[1], partner):
        pl.semaphore_signal(barrier, inc=1, **to(t))
    loads = [pltpu.make_async_copy(s, d, w_sem.at[i]) for i, (s, d) in enumerate(((wg_ref, wg), (wu_ref, wu), (wd_ref, wd)))]
    for c in loads:
        c.start()
    pl.semaphore_wait(barrier, 3)

    for g in range(PARTS):
        for r in range(2):
            gather(0, g, r, x_ref).start()
    for g in range(PARTS):
        share(0, g, x_ref).start()
    run[1] = jnp.zeros_like(run[1])
    for g in range(PARTS):
        share(0, g, x_ref).wait_recv()
    load_partner(0).start()
    loads[0].wait()
    loads[1].wait()

    @pl.loop(0, n + 1)
    def _(q):
        s = q % 2

        @pl.when(q < n)
        def _():
            @pl.when(q < n - 1)
            def _():
                load_partner(0).wait()

                @pl.loop(0, PARTS)
                def _(i):
                    up(xp, 3, i)

                    @pl.when((q != 1) | (i == 0))
                    def _():
                        advance(q + 1, jnp.where(q == 1, 1, i))

            @pl.when((q != 2) & (q + 1 < n))
            def _():
                load_own(q + 1).start()

            @pl.when(q == 0)
            def _():
                loads[2].wait()

            @pl.when(q >= 3)
            def _():
                pl.semaphore_wait(pt_free, 1)

            @pl.loop(0, PIECES)
            def _(p):
                @pl.when(q >= 1)
                def _():
                    pass_term(0, p).wait_send()

                outp[p] = down(3, p).astype(BF16)

                @pl.when(q == 0)
                def _():
                    pass_first(p).start()

                @pl.when(q >= 1)
                def _():
                    pass_term(s, p).start()

        @pl.when((q != 1) & (q < n - 1))
        def _():
            @pl.loop(jnp.where(q == 2, 2, q + 1), q + 2)
            def _(u):
                load_own(0, x_ref).wait()

                @pl.loop(0, jnp.where(q == n - 2, 1, PARTS))
                def _(i):
                    up(xo, u % 2, i)

                    @pl.when((u == 1) & (i == 0))
                    def _():
                        advance(2, 0)
                        await_partner(1)

                @pl.when(u == 2)
                def _():
                    load_own(3).start()

        @pl.when(q == SPARE)
        def _():
            load_own(0, x_ref).start()
            load_own(0, x_ref).wait()

            @pl.loop(0, PARTS)
            def _(i):
                up(xo, 2, i)

        @pl.when((q >= 1) & (q + 1 < n))
        def _():
            await_partner(q + 1)

        @pl.when(q >= 1)
        def _():
            h = jnp.where(q == n, 2, s)

            @pl.when(q == n)
            def _():
                load_first().wait()

                @pl.loop(0, PIECES)
                def _(p):
                    pass_term(0, p).wait_send()

                @pl.loop(0, n)
                def _(d):
                    for g in range(PARTS):
                        share(d, g).wait_send()

                        @pl.when(d < n - 1)
                        def _():
                            for r in range(2):
                                gather(d, g, r).wait_send()

            @pl.when((q >= 2) & (q < n))
            def _():
                for r in range(2):
                    pl.semaphore_wait(run_free.at[r], 1)

            tail = q == n - 2

            @pl.loop(0, jnp.where(tail, 3, 1))
            def _(k):
                @pl.loop(jnp.where(tail, jnp.maximum(2 * k - 1, 0), 0), jnp.where(tail, 2 * k + 1, PIECES))
                def _(p):
                    @pl.when(q >= 2)
                    def _():
                        for r in range(2):
                            pass_sum(q, p, r).wait_send()

                    @pl.when(q >= 2)
                    def _():
                        for r in range(2):
                            pass_sum(q + 1, p, r).wait_recv()

                    @pl.when(q < n)
                    def _():
                        pass_term(s, p).wait_recv()

                    total = (down(h, p) + run[s, p].astype(F32) + pt[s, p].astype(F32)).astype(BF16)

                    @pl.when(q < n)
                    def _():
                        out[p] = total
                        for r in range(2):
                            pass_sum(q, p, r).start()

                    @pl.when(q == n)
                    def _():
                        y_ref[:, cols(p, nb)] = total

                @pl.when(tail & (k == 0))
                def _():
                    up(xo, (n - 1) % 2, 1)
                    load_partner(0).wait()

                @pl.when(tail & (k > 0))
                def _():
                    up(xp, 3, k - 1)

            @pl.when(q < n - 1)
            def _():
                for r in range(2):
                    pl.semaphore_signal(run_free.at[r], inc=1, **to(rings[r][1]))

            @pl.when(q < n - 2)
            def _():
                pl.semaphore_signal(pt_free, inc=1, **to(partner))

            @pl.when(q == n - 2)
            def _():
                for p in range(PIECES):
                    pass_first(p).wait_recv()
                load_first().start()


def solution(mesh):
    n = mesh.shape["tp"] // 2
    side = math.isqrt(n)

    def step(x, w_gate, w_up, w_down):
        rows, depth = x.shape
        width = w_gate.shape[1]
        hbm = pl.BlockSpec(memory_space=pltpu.HBM)
        dma, flag = pltpu.SemaphoreType.DMA, pltpu.SemaphoreType.REGULAR

        def sums(*slots):
            return pltpu.VMEM((*slots, PIECES, rows, depth // PIECES), BF16)

        y, *_ = pl.pallas_call(
            functools.partial(kernel, n, side),
            out_shape=(
                jax.ShapeDtypeStruct((rows, depth), BF16),
                jax.ShapeDtypeStruct((n, rows, depth), BF16),
                jax.ShapeDtypeStruct((n, rows, depth), BF16),
                jax.ShapeDtypeStruct((PIECES, rows, depth // PIECES), BF16),
            ),
            in_specs=[hbm] * 4,
            out_specs=(pl.BlockSpec(memory_space=pltpu.VMEM), hbm, hbm, hbm),
            scratch_shapes=[
                pltpu.VMEM((depth, width), BF16),
                pltpu.VMEM((depth, width), BF16),
                pltpu.VMEM((width, depth), BF16),
                pltpu.VMEM((rows, depth), BF16),
                pltpu.VMEM((rows, depth), BF16),
                pltpu.VMEM((4, rows, width), BF16),
                sums(2), sums(2), sums(), sums(),
                dma((3,)), dma, dma, dma,
                dma((n, PARTS, 2)), dma((n, PARTS, 2)), dma((n, PARTS)), dma((n, PARTS)),
                dma((PIECES, 2)), dma((2, PIECES, 2)), dma((PIECES,)), dma((3, PIECES)),
                flag((2,)), flag,
            ],
            compiler_params=pltpu.CompilerParams(collective_id=0, has_side_effects=True, vmem_limit_bytes=int(51.75 * 2**20)),
            cost_estimate=pl.CostEstimate(
                flops=6 * 2 * n * rows * depth * width, bytes_accessed=8 * 2 * n * rows * depth, transcendentals=0
            ),
            name="mlp",
        )(x, w_gate, w_up, w_down)
        return y

    return jax.shard_map(
        step,
        mesh=mesh,
        in_specs=(P(("dp", "tp"), None), P(None, "tp"), P(None, "tp"), P("tp", None)),
        out_specs=P(("dp", "tp"), None),
        check_vma=False,
    )
```

```python
import functools
import math

import jax
import jax.numpy as jnp
from jax import lax
from jax.experimental import pallas as pl
from jax.experimental.pallas import tpu as pltpu
from jax.sharding import PartitionSpec as P

MESH = pl.DeviceIdType.MESH
BF16 = jnp.bfloat16
F32 = jnp.float32
PARTS = 2
PIECES = 5
SPARE = 4


def neighbours(tp, side):
    core, chip = tp % 2, tp // 2
    x, y = chip // side, chip % side
    last = ((x + y) % side + 1) // side
    first = (side - (x + y) % side) // side

    def at(u, v):
        return (u * side + v) * 2 + core

    a = (at((x + last) % side, (y + 1 - last) % side), at((x + side - first) % side, (y + side - 1 + first) % side))
    b = (at((x + 1 - last) % side, (y + last) % side), at((x + side - 1 + first) % side, (y + side - first) % side))
    turn = lambda p: (p[0] + core * (p[1] - p[0]), p[1] + core * (p[0] - p[1]))
    return turn(a), turn(b), tp + 1 - 2 * core


def kernel(
    n, side,
    x_ref, wg_ref, wu_ref, wd_ref,
    y_ref, xg_ref, xp_ref, pt0_ref,
    wg, wu, wd, xo, xp, hid, run, pt, out, outp,
    w_sem, xo_sem, xp_sem, pt0_sem, ag_send, ag_recv, sh_send, sh_recv, run_send, run_recv, pt_send, pt_recv, run_free, pt_free,
):
    rows, depth = x_ref.shape
    half = rows // 2
    na, nb, nc = hid.shape[2] // PARTS, depth // PIECES, depth // PARTS
    dp, tp = lax.axis_index("dp"), lax.axis_index("tp")
    ring_a, ring_b, partner = neighbours(tp, side)
    rings = (ring_a, ring_b)

    def to(t):
        return dict(device_id=(dp, t), device_id_type=MESH)

    def span(r):
        return pl.ds(r * half, half)

    def cols(i, size):
        return pl.ds(pl.multiple_of(i * size, size), size)

    def gather(d, g, r, src=None):
        return pltpu.make_async_remote_copy(
            (xg_ref.at[d] if src is None else src).at[span(r), cols(g, nc)], xg_ref.at[d + 1, span(r), cols(g, nc)],
            ag_send.at[d, g, r], ag_recv.at[d + 1, g, r], **to(rings[r][0]),
        )

    def share(d, g, src=None):
        return pltpu.make_async_remote_copy(
            (xg_ref.at[d] if src is None else src).at[:, cols(g, nc)], xp_ref.at[d, :, cols(g, nc)],
            sh_send.at[d, g], sh_recv.at[d, g], **to(partner),
        )

    def load_own(d, src=None):
        return pltpu.make_async_copy(xg_ref.at[d] if src is None else src, xo, xo_sem)

    def load_partner(d):
        return pltpu.make_async_copy(xp_ref.at[d], xp, xp_sem)

    def pass_sum(q, p, r):
        t = (q + 1) % 2
        return pltpu.make_async_remote_copy(
            out.at[p, span(r)], run.at[t, p, span(r)], run_send.at[p, r], run_recv.at[t, p, r], **to(rings[r][0])
        )

    def pass_term(t, p):
        return pltpu.make_async_remote_copy(outp.at[p], pt.at[t, p], pt_send.at[p], pt_recv.at[t, p], **to(partner))

    def pass_first(p):
        return pltpu.make_async_remote_copy(outp.at[p], pt0_ref.at[p], pt_send.at[p], pt_recv.at[2, p], **to(partner))

    def load_first():
        return pltpu.make_async_copy(pt0_ref, pt.at[0], pt0_sem)

    def up(x, slot, i):
        c = cols(i, na)
        gate = jnp.dot(x[...], wg[:, c], preferred_element_type=F32)
        up = jnp.dot(x[...], wu[:, c], preferred_element_type=F32)
        hid[slot, :, c] = (jax.nn.silu(gate) * up).astype(BF16)

    def advance(d, g):
        @pl.when(d < n)
        def _():
            for r in range(2):
                gather(d - 1, g, r).wait_recv()

            @pl.when(d + 1 < n)
            def _():
                for r in range(2):
                    gather(d, g, r).start()

            share(d, g).start()

    def await_partner(d):
        for g in range(PARTS):
            share(d, g).wait_recv()
        load_partner(d).start()

    def down(slot, p):
        return jnp.dot(hid[slot], wd[:, cols(p, nb)], preferred_element_type=F32)

    barrier = pltpu.get_barrier_semaphore()
    for t in (ring_a[1], ring_b[1], partner):
        pl.semaphore_signal(barrier, inc=1, **to(t))
    loads = [pltpu.make_async_copy(s, d, w_sem.at[i]) for i, (s, d) in enumerate(((wg_ref, wg), (wu_ref, wu), (wd_ref, wd)))]
    for c in loads:
        c.start()
    pl.semaphore_wait(barrier, 3)

    for g in range(PARTS):
        for r in range(2):
            gather(0, g, r, x_ref).start()
    for g in range(PARTS):
        share(0, g, x_ref).start()
    run[1] = jnp.zeros_like(run[1])
    for g in range(PARTS):
        share(0, g, x_ref).wait_recv()
    load_partner(0).start()
    loads[0].wait()
    loads[1].wait()

    @pl.loop(0, n + 1)
    def _(q):
        s = q % 2

        @pl.when(q < n)
        def _():
            @pl.when(q < n - 1)
            def _():
                load_partner(0).wait()

                @pl.loop(0, PARTS)
                def _(i):
                    up(xp, 3, i)

                    @pl.when((q == 0) | (q == 1) & (i == 0))
                    def _():
                        advance(q + 1, jnp.where(q == 1, 1, i))

            @pl.when(q == 0)
            def _():
                loads[2].wait()

            @pl.when(q >= 3)
            def _():
                pl.semaphore_wait(pt_free, 1)

            @pl.loop(0, PIECES)
            def _(p):
                @pl.when(q >= 1)
                def _():
                    pass_term(0, p).wait_send()

                outp[p] = down(3, p).astype(BF16)

                @pl.when(q == 0)
                def _():
                    pass_first(p).start()

                @pl.when(q >= 1)
                def _():
                    pass_term(s, p).start()

            @pl.when(q >= 2)
            def _():
                for g in range(PARTS):
                    advance(q + 1, g)

            @pl.when((q != 2) & (q + 1 < n))
            def _():
                load_own(q + 1).start()

        @pl.when((q != 1) & (q < n - 1))
        def _():
            @pl.loop(jnp.where(q == 2, 2, q + 1), q + 2)
            def _(u):
                load_own(0, x_ref).wait()

                @pl.loop(0, jnp.where(q == n - 2, 1, PARTS))
                def _(i):
                    up(xo, u % 2, i)

                    @pl.when((u == 1) & (i == 0))
                    def _():
                        advance(2, 0)
                        await_partner(1)

                @pl.when(u == 2)
                def _():
                    load_own(3).start()

        @pl.when(q == SPARE)
        def _():
            load_own(0, x_ref).start()
            load_own(0, x_ref).wait()

            @pl.loop(0, PARTS)
            def _(i):
                up(xo, 2, i)

        @pl.when((q >= 1) & (q + 1 < n))
        def _():
            await_partner(q + 1)

        @pl.when(q >= 1)
        def _():
            h = jnp.where(q == n, 2, s)

            @pl.when(q == n)
            def _():
                load_first().wait()

                @pl.loop(0, PIECES)
                def _(p):
                    pass_term(0, p).wait_send()

                @pl.loop(0, n)
                def _(d):
                    for g in range(PARTS):
                        share(d, g).wait_send()

                        @pl.when(d < n - 1)
                        def _():
                            for r in range(2):
                                gather(d, g, r).wait_send()

            @pl.when((q >= 2) & (q < n))
            def _():
                for r in range(2):
                    pl.semaphore_wait(run_free.at[r], 1)

            tail = q == n - 2

            @pl.loop(0, jnp.where(tail, 3, 1))
            def _(k):
                @pl.loop(jnp.where(tail, jnp.maximum(2 * k - 1, 0), 0), jnp.where(tail, 2 * k + 1, PIECES))
                def _(p):
                    @pl.when(q >= 2)
                    def _():
                        for r in range(2):
                            pass_sum(q, p, r).wait_send()

                    @pl.when(q >= 2)
                    def _():
                        for r in range(2):
                            pass_sum(q + 1, p, r).wait_recv()

                    @pl.when(q < n)
                    def _():
                        pass_term(s, p).wait_recv()

                    total = (down(h, p) + run[s, p].astype(F32) + pt[s, p].astype(F32)).astype(BF16)

                    @pl.when(q < n)
                    def _():
                        out[p] = total
                        for r in range(2):
                            pass_sum(q, p, r).start()

                    @pl.when(q == n)
                    def _():
                        y_ref[:, cols(p, nb)] = total

                @pl.when(tail & (k == 0))
                def _():
                    up(xo, (n - 1) % 2, 1)
                    load_partner(0).wait()

                @pl.when(tail & (k > 0))
                def _():
                    up(xp, 3, k - 1)

            @pl.when(q < n - 1)
            def _():
                for r in range(2):
                    pl.semaphore_signal(run_free.at[r], inc=1, **to(rings[r][1]))

            @pl.when(q < n - 2)
            def _():
                pl.semaphore_signal(pt_free, inc=1, **to(partner))

            @pl.when(q == n - 2)
            def _():
                for p in range(PIECES):
                    pass_first(p).wait_recv()
                load_first().start()


def solution(mesh):
    n = mesh.shape["tp"] // 2
    side = math.isqrt(n)

    def step(x, w_gate, w_up, w_down):
        rows, depth = x.shape
        width = w_gate.shape[1]
        hbm = pl.BlockSpec(memory_space=pltpu.HBM)
        dma, flag = pltpu.SemaphoreType.DMA, pltpu.SemaphoreType.REGULAR

        def sums(*slots):
            return pltpu.VMEM((*slots, PIECES, rows, depth // PIECES), BF16)

        y, *_ = pl.pallas_call(
            functools.partial(kernel, n, side),
            out_shape=(
                jax.ShapeDtypeStruct((rows, depth), BF16),
                jax.ShapeDtypeStruct((n, rows, depth), BF16),
                jax.ShapeDtypeStruct((n, rows, depth), BF16),
                jax.ShapeDtypeStruct((PIECES, rows, depth // PIECES), BF16),
            ),
            in_specs=[hbm] * 4,
            out_specs=(pl.BlockSpec(memory_space=pltpu.VMEM), hbm, hbm, hbm),
            scratch_shapes=[
                pltpu.VMEM((depth, width), BF16),
                pltpu.VMEM((depth, width), BF16),
                pltpu.VMEM((width, depth), BF16),
                pltpu.VMEM((rows, depth), BF16),
                pltpu.VMEM((rows, depth), BF16),
                pltpu.VMEM((4, rows, width), BF16),
                sums(2), sums(2), sums(), sums(),
                dma((3,)), dma, dma, dma,
                dma((n, PARTS, 2)), dma((n, PARTS, 2)), dma((n, PARTS)), dma((n, PARTS)),
                dma((PIECES, 2)), dma((2, PIECES, 2)), dma((PIECES,)), dma((3, PIECES)),
                flag((2,)), flag,
            ],
            compiler_params=pltpu.CompilerParams(collective_id=0, has_side_effects=True, vmem_limit_bytes=int(51.75 * 2**20)),
            cost_estimate=pl.CostEstimate(
                flops=6 * 2 * n * rows * depth * width, bytes_accessed=8 * 2 * n * rows * depth, transcendentals=0
            ),
            name="mlp",
        )(x, w_gate, w_up, w_down)
        return y

    return jax.shard_map(
        step,
        mesh=mesh,
        in_specs=(P(("dp", "tp"), None), P(None, "tp"), P(None, "tp"), P("tp", None)),
        out_specs=P(("dp", "tp"), None),
        check_vma=False,
    )
```
